32 devices in a mesh: cuts: 4 (over x, core), exp: 2 (over y), fsdp: 4 (over z).
Axes of the slice: x: 2, y: 2, z: 4, core: 2. Of those that a mesh axis runs over, the one named last changes fastest.
Arguments:
- tokens: bfloat16 [4096, 4096], P(('cuts', 'exp', 'fsdp')), may hold values from -6 to 6
- out_grad: bfloat16 [4096, 4096], P(('cuts', 'exp', 'fsdp')), may hold values from -6 to 6
- expert_ids: int32 [4096, 2], P(('cuts', 'exp', 'fsdp')), may hold values from 0 to 7, as said below
- gate_probs: bfloat16 [4096, 2], P(('cuts', 'exp', 'fsdp')), may hold values from 0.049804688 to 0.94921875
- params: float32 [3, 8, 4096, 256], P(None, 'exp', ('cuts', 'fsdp')), may hold values from -0.1875 to 0.1875
- moment_first: float32 [3, 8, 4096, 256], P(None, 'exp', ('cuts', 'fsdp')), may hold values from -60 to 60
- moment_second: float32 [3, 8, 4096, 256], P(None, 'exp', ('cuts', 'fsdp')), may hold values from 64 to 1024
Outputs:
- token_grad: bfloat16 [4096, 4096], P(('cuts', 'exp', 'fsdp'))
- gate_grad: bfloat16 [4096, 2], P(('cuts', 'exp', 'fsdp'))
- new_params: float32 [3, 8, 4096, 256], P(None, 'exp', ('cuts', 'fsdp'))
- new_first: float32 [3, 8, 4096, 256], P(None, 'exp', ('cuts', 'fsdp'))
- new_second: float32 [3, 8, 4096, 256], P(None, 'exp', ('cuts', 'fsdp'))
The draws below stay inside these ranges and needn't reach their ends.
Inputs may be any that keep to these rules, and one draw needn't show every extreme that they name: `expert_ids`: the two ids of a token differ. Among the tokens of one device no expert is named more than 40 times. Each device names some expert exactly 40 times, and the devices that share their cuts and fsdp indices have one such expert in common.
All inputs are finite; a program needn't handle non-finite values.
Results may differ from the reference program's by a relative error of at most 0.0079.
Values may be sent and summed in bfloat16 or wider, within the bound.
No kernel may reach another device: no remote copies, remote signals or barrier semaphores. Data moves between devices by JAX's collectives and lax.ppermute only.
A program may use at most 192 MiB of HBM per device.

```python
import math
import jax
import jax.numpy as jnp
from jax import lax

D = 4096
EXPERTS = 8
F = 256
TOK_DEV = 128
CAP = 40
SENDERS = 2
SHARDS = 4
TOKENS = 4096


def draw_expert_ids(key, part):
    blocks = TOKENS // TOK_DEV
    unit = TOK_DEV // 32
    groups = blocks // SENDERS
    pattern = jnp.array([10, 9, 9, 8, 8, 7, 7, 6], jnp.int32) * unit
    shifts = jax.random.randint(jax.random.fold_in(key, 11), (blocks, 3), -unit, unit + 1).astype(jnp.int32)
    nothing = jnp.zeros((blocks,), jnp.int32)
    delta = jnp.stack([nothing, shifts[:, 0], -shifts[:, 0], shifts[:, 1], -shifts[:, 1], shifts[:, 2], -shifts[:, 2], nothing], axis=1)
    counts = pattern[None, :] + delta
    ends = jnp.cumsum(counts, axis=1)
    position = jnp.arange(2 * TOK_DEV, dtype=jnp.int32)
    pattern_slot = jnp.sum((position[None, :, None] >= ends[:, None, :]).astype(jnp.int32), axis=2)
    block_number = jnp.arange(blocks, dtype=jnp.int32)
    group_number = block_number // (SENDERS * SHARDS) * SHARDS + block_number % SHARDS
    full_expert = jax.random.randint(jax.random.fold_in(key, 12), (groups,), 0, 8).astype(jnp.int32)[group_number]
    order_keys = jax.random.split(jax.random.fold_in(key, 13), blocks)
    orders = jax.vmap(lambda one: jax.random.permutation(one, 8))(order_keys).astype(jnp.int32)
    labels = (orders - orders[:, :1] + full_expert[:, None]) % 8
    named = jnp.take_along_axis(labels, pattern_slot, axis=1)
    first_half = named[:, :TOK_DEV]
    second_half = named[:, TOK_DEV:]
    flipped = jax.random.randint(jax.random.fold_in(key, 14), (blocks, TOK_DEV), 0, 2).astype(jnp.int32)
    paired = jnp.stack([jnp.where(flipped == 1, second_half, first_half), jnp.where(flipped == 1, first_half, second_half)], axis=-1)
    shuffle_keys = jax.random.split(jax.random.fold_in(key, 15), blocks)
    shuffles = jax.vmap(lambda one: jax.random.permutation(one, TOK_DEV))(shuffle_keys).astype(jnp.int32)
    paired = jnp.take_along_axis(paired, shuffles[:, :, None], axis=1)
    return paired.reshape(TOKENS, 2).astype(jnp.int32)


def with_spikes(values, stream_key, source, target, parts, factor):
    def block_of(dim):
        return (jnp.arange(values.shape[dim]) // (values.shape[dim] // parts)).reshape((-1,) + (1,) * (values.ndim - 1 - dim))

    near = jax.random.permutation(stream_key, parts)[block_of(target)]
    other_side = (block_of(target) + parts // 2) % parts
    return jnp.where((block_of(source) == near) | (block_of(source) == other_side), factor * values, values)


def steps_of(key, extent, shards, low, top_value):
    factor_of, own = 1.0, jax.random.fold_in(key, 6)
    for dim, shards_of in shards:
        draws = jnp.exp(jax.random.uniform(jax.random.fold_in(own, dim), (shards_of,), jnp.float32, low / len(shards), top_value / len(shards)))
        factor_of = factor_of * jnp.repeat(draws, extent[dim] // shards_of).reshape([-1 if axis == dim else 1 for axis in range(len(extent))])
    return factor_of


def noise(rng, shape, scale, most, cuts=(), kind=jnp.bfloat16):
    result = jax.random.normal(rng, shape, jnp.float32) * scale
    if len(cuts) > 0:
        result = steps_of(rng, shape, cuts, -0.22, 0.18) * result
    return jnp.clip(result, min=-most, max=most).astype(kind)


def heavy_noise(key, extent, scale, most, cuts, heavy, kind=jnp.bfloat16):
    result = scale * jax.random.normal(key, extent, jnp.float32)
    if cuts:
        result = result * steps_of(key, extent, cuts, -0.22, 0.18)
    return jnp.clip(with_spikes(result, jax.random.fold_in(key, 3), *heavy), -most, most).astype(kind)


def setup_inputs(seed: int = 0) -> dict:
    splits = jax.random.split(jax.random.key(seed), 8)
    tokens = noise(splits[0], (TOKENS, D), 1.0, 6.0, ((0, 32),))
    out_grad = heavy_noise(splits[1], (TOKENS, D), 1.0, 6.0, ((0, 32),), (0, 1, 32, 2.75))
    expert_ids = draw_expert_ids(jax.random.fold_in(splits[7], 71), 0)
    gate_probs = jnp.clip(0.049804688 + 0.89941406 * jax.random.uniform(splits[3], (TOKENS, 2), jnp.float32) ** steps_of(splits[3], (TOKENS, 2), ((0, 32),), -0.2, 0.2), 0.049804688, 0.94921875).astype(jnp.bfloat16)
    params = noise(splits[4], (3, EXPERTS, D, F), (D // 4) ** -0.5, 0.1875, ((1, 2), (2, 16)), jnp.float32)
    moment_first = noise(splits[5], (3, EXPERTS, D, F), 10.0, 60.0, ((1, 2), (2, 16)), jnp.float32)
    moment_second = jnp.clip(jnp.exp(math.log(1024.0) - 2.7725887 * jax.random.uniform(splits[6], (3, EXPERTS, D, F), jnp.float32) ** steps_of(splits[6], (3, EXPERTS, D, F), ((1, 2), (2, 16)), -0.2, 0.2)), 64.0, 1024.0)
    return dict(tokens=tokens, out_grad=out_grad, expert_ids=expert_ids, gate_probs=gate_probs, params=params, moment_first=moment_first, moment_second=moment_second)


decay_first = 0.9
decay_second = 0.95
correct_first = 1.0 - 0.9 ** 10
correct_second = 1.0 - 0.95 ** 10
epsilon = 1e-08
learn_rate = 0.0003
weight_decay = 0.1

def adam_update(params, gradient, moment_first, moment_second):
    new_first = decay_first * moment_first + (1.0 - decay_first) * gradient
    new_second = decay_second * moment_second + (1.0 - decay_second) * gradient * gradient
    stepped = new_first / correct_first / (jnp.sqrt(new_second / correct_second) + epsilon)
    new_params = params - learn_rate * (stepped + weight_decay * params)
    return (new_params, new_first, new_second)

def reference(tokens, out_grad, expert_ids, gate_probs, params, moment_first, moment_second):
    weights = params.astype(jnp.bfloat16)
    token_count = tokens.shape[0]
    slots_most = CAP * (TOKENS // TOK_DEV)
    flat_ids = expert_ids.reshape(-1)
    flat_gate = gate_probs.reshape(-1)

    def expert_step(totals, expert):
        token_acc, gate_acc = totals
        chosen = flat_ids == expert
        picked = jnp.nonzero(chosen, size=slots_most, fill_value=0)[0].astype(jnp.int32)
        filled = jnp.arange(slots_most, dtype=jnp.int32) < jnp.sum(chosen.astype(jnp.int32))
        token_rows = picked // 2
        inputs = tokens[token_rows]
        upstream = out_grad[token_rows]
        gate_values = jnp.where(filled, flat_gate[picked], jnp.zeros((), flat_gate.dtype)).astype(jnp.float32)[:, None]
        w_gate = weights[0, expert]
        w_up = weights[1, expert]
        w_down = weights[2, expert]
        pre_gate = jnp.dot(inputs, w_gate, preferred_element_type=jnp.float32)
        pre_up = jnp.dot(inputs, w_up, preferred_element_type=jnp.float32)
        sigmoid_gate = jax.nn.sigmoid(pre_gate)
        activated = pre_gate * sigmoid_gate
        hidden = activated * pre_up
        projected = jnp.dot(upstream, w_down, preferred_element_type=jnp.float32)
        slot_gate = lax.optimization_barrier(jnp.sum(hidden * projected, axis=1)).astype(jnp.bfloat16)
        delta_hidden = gate_values * projected
        delta_gate = (delta_hidden * pre_up * sigmoid_gate * (1.0 + pre_gate * (1.0 - sigmoid_gate))).astype(jnp.bfloat16)
        delta_up = (delta_hidden * activated).astype(jnp.bfloat16)
        scaled = (gate_values * upstream.astype(jnp.float32)).astype(jnp.bfloat16)
        slot_grads = (jnp.dot(delta_gate, w_gate.T, preferred_element_type=jnp.float32) + jnp.dot(delta_up, w_up.T, preferred_element_type=jnp.float32)).astype(jnp.bfloat16)
        grad_gate = jnp.dot(inputs.T, delta_gate, preferred_element_type=jnp.float32)
        grad_up = jnp.dot(inputs.T, delta_up, preferred_element_type=jnp.float32)
        grad_down = jnp.dot(scaled.T, hidden.astype(jnp.bfloat16), preferred_element_type=jnp.float32)
        token_acc = token_acc.at[token_rows].add(jnp.where(filled[:, None], slot_grads.astype(jnp.float32), jnp.zeros((), jnp.float32)))
        gate_acc = gate_acc.at[picked].add(jnp.where(filled, slot_gate.astype(jnp.float32), jnp.zeros((), jnp.float32)))
        return ((token_acc, gate_acc), jnp.stack([grad_gate, grad_up, grad_down]))
    start = (jnp.zeros(tokens.shape, jnp.float32), jnp.zeros((token_count * 2,), jnp.float32))
    (token_acc, gate_acc), gradient = lax.scan(expert_step, start, jnp.arange(EXPERTS, dtype=jnp.int32))
    gradient = jnp.transpose(gradient, (1, 0, 2, 3))
    new_params, new_first, new_second = adam_update(params, gradient, moment_first, moment_second)
    return (token_acc.astype(jnp.bfloat16), gate_acc.reshape(token_count, 2).astype(jnp.bfloat16), new_params, new_first, new_second)
```

```python
import functools

import jax
import jax.numpy as jnp
from jax import lax
from jax.experimental import pallas as pl
from jax.experimental.pallas import tpu as pltpu
from jax.sharding import Mesh
from jax.sharding import PartitionSpec as P

EXPERTS = 8
ROWS = ("x", "fsdp")

decay_first = 0.9
decay_second = 0.95
correct_first = 1.0 - 0.9**10
correct_second = 1.0 - 0.95**10
epsilon = 1e-08
learn_rate = 0.0003
weight_decay = 0.1


bf16 = jnp.bfloat16
f32 = jnp.float32


def adam_update(params, gradient, moment_first, moment_second):
    new_first = decay_first * moment_first + (1.0 - decay_first) * gradient
    new_second = decay_second * moment_second + (1.0 - decay_second) * gradient * gradient
    stepped = new_first / correct_first / (jnp.sqrt(new_second / correct_second) + epsilon)
    new_params = params - learn_rate * (stepped + weight_decay * params)
    return (new_params, new_first, new_second)


def dot(left, right, left_dim=1, right_dim=0):
    return lax.dot_general(left, right, (((left_dim,), (right_dim,)), ((), ())), preferred_element_type=f32)


def place_pairs(targets_ref, source, slots):
    targets = targets_ref[source]
    return (lax.broadcasted_iota(jnp.int32, (slots, targets.shape[1]), 0) == targets).astype(bf16)


def place_tokens(targets_ref, source, slots):
    pairs = place_pairs(targets_ref, source, slots)
    half = pairs.shape[1] // 2
    return pairs[:, :half] + pairs[:, half:]


def expert_weight(pieces, array, expert):
    local = pieces[0].shape[1]
    return pieces[expert // local][array, expert % local]


def shifts():
    return [(dx, dz) for dx in range(lax.axis_size("x")) for dz in range(lax.axis_size("fsdp"))]


def source_index(place_ref, dx, dz):
    x_count, z_count = lax.axis_size("x"), lax.axis_size("fsdp")
    return (place_ref[0] + dx) % x_count * z_count + (place_ref[2] + dz) % z_count


def column_starts(place_ref, dx, dz, rows):
    x_count, z_count = lax.axis_size("x"), lax.axis_size("fsdp")
    x = (place_ref[0] + x_count - dx) % x_count
    z = (place_ref[2] + z_count - dz) % z_count
    return [pl.multiple_of(((x * 2 + core) * z_count + z) * rows, rows) for core in (place_ref[1], 1 - place_ref[1])]


def split_kernel(steps, place_ref, array_ref, *piece_refs):
    rows = piece_refs[0].shape[1] // 2
    for (dx, dz), piece_ref in zip(steps, piece_refs):
        for half, start in enumerate(column_starts(place_ref, dx, dz, rows)):
            piece_ref[:, half * rows : (half + 1) * rows] = array_ref[:, pl.ds(start, rows)]


def join_kernel(steps, place_ref, *refs):
    piece_refs, array_ref = refs[:-1], refs[-1]
    rows = piece_refs[0].shape[1] // 2
    for (dx, dz), piece_ref in zip(steps, piece_refs):
        for half, start in enumerate(column_starts(place_ref, dx, dz, rows)):
            array_ref[:, pl.ds(start, rows)] = piece_ref[:, half * rows : (half + 1) * rows]


def forward_kernel(pieces, steps, place_ref, targets_ref, *refs):
    x_refs, refs = refs[: len(steps)], refs[len(steps) :]
    own, pair = refs[:pieces], refs[pieces : 2 * pieces]
    refs = refs[2 * pieces :]
    arrays, _, rows, units = own[0].shape
    placed_ref, out_refs, part_ref = refs[0], refs[1:-1], refs[-1]
    sources = len(steps)
    capacity = placed_ref.shape[1] // sources
    slots = EXPERTS * capacity
    z_count = out_refs[0].shape[0]
    where = [source_index(place_ref, dx, dz) for dx, dz in steps]
    for n in range(sources):
        placed = dot(place_tokens(targets_ref, where[n], slots), x_refs[n][...]).astype(bf16)
        for e in range(EXPERTS):
            placed_ref[e, n * capacity : (n + 1) * capacity, :] = placed[e * capacity : (e + 1) * capacity]
    for a in range(arrays):
        for e in range(EXPERTS):
            part = dot(placed_ref[e, :, :rows], expert_weight(own, a, e))
            part = part + dot(placed_ref[e, :, rows:], expert_weight(pair, a, e))
            part_ref[e] = part.astype(bf16)
        for n in range(sources):
            part = jnp.concatenate([part_ref[e, n * capacity : (n + 1) * capacity, :] for e in range(EXPERTS)], axis=0)
            part = dot(place_pairs(targets_ref, where[n], slots), part, 0, 0).astype(bf16)
            out_refs[a * (sources // z_count) + n // z_count][n % z_count] = part


def token_kernel(pieces, steps, place_ref, targets_ref, *refs):
    sources = len(steps)
    gate_refs, up_refs, refs = refs[:sources], refs[sources : 2 * sources], refs[2 * sources :]
    own, pair, refs = refs[:pieces], refs[pieces : 2 * pieces], refs[2 * pieces :]
    delta_ref, token_refs, slot_ref = refs[0], refs[1:-1], refs[-1]
    capacity = delta_ref.shape[1] // sources
    slots = EXPERTS * capacity
    _, _, rows, units = own[0].shape
    where = [source_index(place_ref, dx, dz) for dx, dz in steps]
    for n in range(sources):
        pairs = place_pairs(targets_ref, where[n], slots)
        for a, ref in enumerate((gate_refs[n], up_refs[n])):
            placed = dot(pairs, ref[...]).astype(bf16)
            for e in range(EXPERTS):
                delta_ref[e, n * capacity : (n + 1) * capacity, a * units : (a + 1) * units] = placed[
                    e * capacity : (e + 1) * capacity
                ]
    for e in range(EXPERTS):
        for h, weights in enumerate((own, pair)):
            part = dot(delta_ref[e, :, :units], expert_weight(weights, 0, e), 1, 1)
            part = part + dot(delta_ref[e, :, units:], expert_weight(weights, 1, e), 1, 1)
            slot_ref[e, :, h * rows : (h + 1) * rows] = part.astype(bf16)
    for n in range(sources):
        part = jnp.concatenate([slot_ref[e, n * capacity : (n + 1) * capacity, :] for e in range(EXPERTS)], axis=0)
        token_refs[n][...] = dot(place_tokens(targets_ref, where[n], slots), part, 0, 0).astype(bf16)


def grad_kernel(placed_ref, delta_ref, own_ref, pair_ref):
    arrays, _, rows, units = own_ref.shape
    for a in range(arrays):
        for e in range(EXPERTS):
            grad = dot(placed_ref[e], delta_ref[e, :, a * units : (a + 1) * units], 0, 0)
            own_ref[a, e] = grad[:rows]
            pair_ref[a, e] = grad[rows:].astype(bf16)


def down_kernel(steps, place_ref, targets_ref, *refs):
    hidden_refs, (placed_ref, own_ref, pair_ref, delta_ref) = refs[: len(steps)], refs[len(steps) :]
    capacity = placed_ref.shape[1] // len(steps)
    slots = EXPERTS * capacity
    for n, (dx, dz) in enumerate(steps):
        pairs = place_pairs(targets_ref, source_index(place_ref, dx, dz), slots)
        placed = dot(pairs, hidden_refs[n][...]).astype(bf16)
        for e in range(EXPERTS):
            delta_ref[e, n * capacity : (n + 1) * capacity, :] = placed[e * capacity : (e + 1) * capacity]
    grad_kernel(placed_ref, delta_ref, own_ref, pair_ref)


def kernel(body, name, operands, outs, scratch=(), place=None):
    in_specs = [pl.BlockSpec(memory_space=pltpu.VMEM)] * len(operands)
    if place is not None:
        in_specs = [pl.BlockSpec(memory_space=pltpu.SMEM)] + in_specs
        operands = [place] + list(operands)
    return pl.pallas_call(
        body,
        in_specs=in_specs,
        out_specs=[pl.BlockSpec(memory_space=pltpu.VMEM)] * len(outs),
        out_shape=[jax.ShapeDtypeStruct(shape, dtype) for shape, dtype in outs],
        scratch_shapes=[pltpu.VMEM(shape, bf16) for shape in scratch],
        compiler_params=pltpu.CompilerParams(vmem_limit_bytes=48 * 2**20),
        name=name,
    )(*operands)


def exchange(blocks, axes):
    return lax.all_to_all(blocks, axes, split_axis=0, concat_axis=0, tiled=True)


def send(array, dx, dz):
    x_count, z_count = lax.axis_size("x"), lax.axis_size("fsdp")
    if dx % x_count == 0 and dz % z_count == 0:
        return array
    pairs = [
        (x * z_count + z, (x + dx) % x_count * z_count + (z + dz) % z_count)
        for x in range(x_count)
        for z in range(z_count)
    ]
    return lax.ppermute(array, ROWS, pairs)


def shifted(array, amount, axis):
    count = lax.axis_size(axis)
    return lax.ppermute(array, axis, [((i + amount) % count, i) for i in range(count)])


def per_device(tokens, out_grad, expert_ids, gate_probs, params, moment_first, moment_second):
    token_count, width = tokens.shape
    local_count, rows, units = params.shape[1:]
    exp_count, x_count, z_count = (lax.axis_size(axis) for axis in ("exp", "x", "fsdp"))
    steps = shifts()
    sources = len(steps)
    capacity = -(-(10 * token_count // 32) // 16) * 16
    slots = sources * capacity
    pairs = 2 * token_count
    place = jnp.stack([lax.axis_index(axis) for axis in ("x", "core", "fsdp")]).astype(jnp.int32)

    def gather(array):
        array = array.astype(bf16)
        own = [array] + [shifted(array, r, "exp") for r in range(1, exp_count)]
        return own, [shifted(piece, 1, "core") for piece in own]

    own_in, pair_in = gather(params[:2])
    own_down, pair_down = gather(params[2:])

    holder = (expert_ids // local_count - lax.axis_index("exp")) % exp_count
    flat_ids = (holder * local_count + expert_ids % local_count).T.reshape(-1)
    onehot = (flat_ids[:, None] == jnp.arange(EXPERTS, dtype=jnp.int32)[None, :]).astype(jnp.int32)
    before = jnp.cumsum(onehot, axis=0) - onehot
    target = flat_ids * capacity + jnp.sum(before * onehot, axis=1)
    targets = exchange(jnp.broadcast_to(target.reshape(1, 1, pairs), (sources, 1, pairs)), ROWS)

    def columns(array, name):
        outs = [((token_count, 2 * rows), bf16)] * sources
        cut = kernel(functools.partial(split_kernel, steps), name, [array], outs, place=place)
        return [send(piece, -dx, -dz) for piece, (dx, dz) in zip(cut, steps)]

    def forward(columns_of, own, pair, name):
        arrays = own[0].shape[0]
        outs = [((EXPERTS, slots, 2 * rows), bf16)] + [((z_count, pairs, units), bf16)] * (arrays * x_count)
        body = functools.partial(forward_kernel, len(own), steps)
        placed, *partial = kernel(
            body, name, [targets, *columns_of, *own, *pair], outs, [(EXPERTS, slots, units)], place
        )
        return placed, [partial[a * x_count : (a + 1) * x_count] for a in range(arrays)]

    def reduce(partial):
        arrived = [partial[0]] + [send(partial[dx], dx, 0) for dx in range(1, x_count)]
        total = 0.0
        for dz in range(z_count):
            part = sum(block[dz].astype(f32) for block in arrived)
            total = total + (part if dz == 0 else send(part.astype(bf16), 0, dz).astype(f32))
        return total

    def gathered(array):
        along = [send(array, 0, -dz) for dz in range(z_count)]
        return [send(along[dz], -dx, 0) for dx, dz in steps]

    inputs, (partial_gate, partial_up) = forward(columns(tokens, "split_tokens"), own_in, pair_in, "forward_in")
    upstream, (partial_down,) = forward(columns(out_grad, "split_upstream"), own_down, pair_down, "forward_down")
    pre_gate = reduce(partial_gate)
    pre_up = reduce(partial_up)
    projected = reduce(partial_down)

    gate_values = gate_probs.T.reshape(-1, 1).astype(f32)
    sigmoid_gate = jax.nn.sigmoid(pre_gate)
    activated = pre_gate * sigmoid_gate
    hidden = activated * pre_up
    gate_grad = jnp.sum(hidden * projected, axis=1).astype(bf16).reshape(2, token_count).T
    delta_hidden = gate_values * projected
    delta_gate = (delta_hidden * pre_up * sigmoid_gate * (1.0 + pre_gate * (1.0 - sigmoid_gate))).astype(bf16)
    delta_up = (delta_hidden * activated).astype(bf16)
    scaled_hidden = (gate_values * hidden).astype(bf16)

    gates, ups, hiddens = gathered(delta_gate), gathered(delta_up), gathered(scaled_hidden)
    outs = [((EXPERTS, slots, 2 * units), bf16)] + [((token_count, 2 * rows), bf16)] * sources
    deltas, *token_pieces = kernel(
        functools.partial(token_kernel, len(own_in), steps),
        "token_grads",
        [targets, *gates, *ups, *own_in, *pair_in],
        outs,
        [(EXPERTS, slots, 2 * rows)],
        place,
    )
    token_pieces = [send(piece, dx, dz) for piece, (dx, dz) in zip(token_pieces, steps)]
    (token_grad,) = kernel(
        functools.partial(join_kernel, steps), "join_tokens", token_pieces, [(tokens.shape, bf16)], place=place
    )

    def grad_outs(arrays):
        return [((arrays, EXPERTS, rows, units), f32), ((arrays, EXPERTS, rows, units), bf16)]

    grads_own, grads_pair = kernel(grad_kernel, "grads_in", [inputs, deltas], grad_outs(2))
    down_own, down_pair = kernel(
        functools.partial(down_kernel, steps),
        "grads_down",
        [targets, *hiddens, upstream],
        grad_outs(1),
        [(EXPERTS, slots, units)],
        place,
    )

    def total(own, pair):
        own = own + shifted(pair, 1, "core").astype(f32)
        gradient = own[:, :local_count]
        for r in range(1, exp_count):
            block = own[:, r * local_count : (r + 1) * local_count].astype(bf16)
            gradient = gradient + shifted(block, exp_count - r, "exp").astype(f32)
        return gradient

    gradient = jnp.concatenate([total(grads_own, grads_pair), total(down_own, down_pair)], axis=0)
    new_params, new_first, new_second = adam_update(params, gradient, moment_first, moment_second)
    return (token_grad, gate_grad, new_params, new_first, new_second)


def solution(mesh):
    cuts, exp, fsdp = (mesh.shape[axis] for axis in ("cuts", "exp", "fsdp"))
    split = Mesh(mesh.devices.reshape(cuts // 2, 2, exp, fsdp), ("x", "core", "exp", "fsdp"))
    rows = P(("x", "core", "exp", "fsdp"), None)
    state = P(None, "exp", ("x", "core", "fsdp"), None)
    return jax.shard_map(
        per_device,
        mesh=split,
        in_specs=(rows, rows, rows, rows, state, state, state),
        out_specs=(rows, rows, state, state, state),
        check_vma=False,
    )
```
